32 devices in a mesh: tm: 8 (over z, y), mp: 4 (over x, core).
Axes of the slice: x: 2, y: 2, z: 4, core: 2. Of those that a mesh axis runs over, the one named last changes fastest.
Arguments:
- latents: float32 [4, 8, 4, 4096], P(None, 'tm'), may hold values from -6 to 6
- noise: float32 [4, 8, 4, 4096], P(None, 'tm'), may hold values from -6 to 6
- start_step: int32 [4], replicated, may hold values from 8 to 999
- slide: int32 [4], replicated, may hold values from 1 to 8, as said below
- w_in: float32 [4, 320], replicated, may hold values from -3 to 3
- w_gate: bfloat16 [320, 1280], P(None, 'mp'), may hold values from -0.3125 to 0.3125
- w_value: bfloat16 [320, 1280], P(None, 'mp'), may hold values from -0.3125 to 0.3125
- w_down: bfloat16 [1280, 320], P('mp'), may hold values from -0.15625 to 0.15625
- w_out: float32 [320, 4], replicated, may hold values from -0.3125 to 0.3125
Outputs:
- next_window: float32 [4, 8, 4, 4096], P(None, 'tm')
- eps: float32 [4, 8, 4, 4096], P(None, 'tm', None, 'mp')
The draws below stay inside these ranges and needn't reach their ends.
Inputs may be any that keep to these rules, and one draw needn't show every extreme that they name: `slide`: some prompt slides by exactly 8, and another by exactly 1.
All inputs are finite; a program needn't handle non-finite values.
Results may differ from the reference program's by a relative error of at most 0.0023.
Values sent between devices are 32-bit elements; how exact they have to be, the bound alone decides.
No kernel may reach another device: no remote copies, remote signals or barrier semaphores. Data moves between devices by JAX's collectives and lax.ppermute only.
A program may use at most 64 MiB of HBM per device.

```python
import math
import jax
import jax.numpy as jnp
from jax import lax

C = 320
FF = 1280
LAT = 4
POS = 4096
PROMPTS = 4
TSTEPS = 1000
WIN = 8
SMAX = 8


def draw_slide(key, part):
    first, second = jax.random.split(jax.random.fold_in(key, 17))
    values = jax.random.randint(first, (PROMPTS,), 1, SMAX + 1)
    order = jax.random.permutation(second, PROMPTS)
    values = jnp.where(order == 0, SMAX, values)
    values = jnp.where(order == 1, 1, values)
    return values.astype(jnp.int32)


def plant(array, own_key, low, top_value):
    longest = array.shape.index(max(array.shape))
    spots = []
    for shift in (0, 1):
        where = [jax.random.randint(jax.random.fold_in(own_key, axis), (), 0, length) for axis, length in enumerate(array.shape)]
        where[longest] = (where[longest] + shift) % array.shape[longest]
        spots.append(tuple(where))
    return array.at[spots[0]].set(low).at[spots[1]].set(top_value)


def block_levels(key, dims, cuts, least, largest):
    level, own = 1.0, jax.random.fold_in(key, 6)
    for position, shards_of in cuts:
        steps = jnp.exp(jax.random.uniform(jax.random.fold_in(own, position), (shards_of,), jnp.float32, least / len(cuts), largest / len(cuts)))
        level = level * jnp.repeat(steps, dims[position] // shards_of).reshape([-1 if axis == position else 1 for axis in range(len(dims))])
    return level


def bell_draw(rng, extent, deviation, bound, pieces=(), kind=jnp.bfloat16):
    loudness = block_levels(rng, extent, pieces, -0.22, 0.18) if pieces else 1.0
    entries = jax.random.normal(rng, extent, jnp.float32) * deviation * loudness
    return jnp.minimum(jnp.maximum(entries, -bound), bound).astype(kind)


def setup_inputs(seed: int = 0) -> dict:
    splits = jax.random.split(jax.random.key(seed), 10)
    latents = bell_draw(splits[0], (PROMPTS, WIN, LAT, POS), 1.0, 6.0, ((1, 8),), jnp.float32)
    noise = bell_draw(splits[1], (PROMPTS, WIN, LAT, POS), 1.0, 6.0, ((1, 8),), jnp.float32)
    start_step = plant(jax.random.randint(splits[2], (PROMPTS,), WIN, TSTEPS), jax.random.fold_in(splits[2], 1), WIN, TSTEPS - 1).astype(jnp.int32)
    slide = draw_slide(jax.random.fold_in(splits[9], 71), 0)
    w_in = bell_draw(splits[4], (LAT, C), LAT ** -0.5, 3.0, (), jnp.float32)
    w_gate = bell_draw(splits[5], (C, FF), C ** -0.5, 0.3125, ((1, 4),))
    w_value = bell_draw(splits[6], (C, FF), C ** -0.5, 0.3125, ((1, 4),))
    w_down = bell_draw(splits[7], (FF, C), FF ** -0.5, 0.15625, ((0, 4),))
    w_out = bell_draw(splits[8], (C, LAT), C ** -0.5, 0.3125, (), jnp.float32)
    return {"latents": latents, "noise": noise, "start_step": start_step, "slide": slide, "w_in": w_in, "w_gate": w_gate, "w_value": w_value, "w_down": w_down, "w_out": w_out}


def plan():
    steps_f = jnp.arange(TSTEPS, dtype=jnp.float32)
    beta = 0.0001 + (0.02 - 0.0001) * steps_f / (TSTEPS - 1)
    abar = jnp.cumprod(1.0 - beta)
    return (beta, abar)

def embed(times):
    half = C // 2
    freq = jnp.exp(-math.log(10000.0) * jnp.arange(half, dtype=jnp.float32) / half)
    angle = times[..., None] * freq
    return jnp.concatenate([jnp.cos(angle), jnp.sin(angle)], axis=-1)

def reference(latents, noise, start_step, slide, w_in, w_gate, w_value, w_down, w_out):
    beta, abar = plan()
    slots = jnp.arange(WIN, dtype=jnp.int32)
    times = start_step[:, None] - slots[None, :]
    beta_t = beta[times][:, :, None, None]
    abar_t = abar[times][:, :, None, None]
    emb = embed(times.astype(jnp.float32)).reshape(PROMPTS * WIN, C)
    items = latents.reshape(PROMPTS * WIN, LAT, POS)

    def denoise(pair):
        latent, vector = pair
        hid = jnp.dot(w_in.T, latent, precision=lax.Precision.HIGHEST) + vector[:, None]
        mean = lax.optimization_barrier(jnp.mean(hid, axis=0))
        var = lax.optimization_barrier(jnp.mean((hid - mean) ** 2, axis=0))
        normed = ((hid - mean) * lax.rsqrt(var + 1e-05)).astype(jnp.bfloat16)
        gate = jnp.dot(w_gate.T, normed, preferred_element_type=jnp.float32)
        value = jnp.dot(w_value.T, normed, preferred_element_type=jnp.float32)
        hidden = (jax.nn.gelu(gate, approximate=False) * value).astype(jnp.bfloat16)
        branch = jnp.dot(w_down.T, hidden, preferred_element_type=jnp.float32)
        return jnp.dot(w_out.T, hid + branch, precision=lax.Precision.HIGHEST)
    eps = lax.map(denoise, (items, emb)).reshape(PROMPTS, WIN, LAT, POS)
    stepped = (latents - beta_t / jnp.sqrt(1.0 - abar_t) * eps) / jnp.sqrt(1.0 - beta_t) + jnp.sqrt(beta_t) * noise
    drift = stepped - latents
    updated = latents[:, :1] + (jnp.cumsum(drift, axis=1) - drift)
    source = jnp.minimum(slots[None, :] + slide[:, None], WIN - 1).astype(jnp.int32)
    next_window = jnp.take_along_axis(updated, source[:, :, None, None], axis=1)
    return (next_window, eps)
```

```python
import math

import jax
import jax.numpy as jnp
import numpy as np
from jax import lax
from jax.experimental import pallas as pl
from jax.experimental.pallas import tpu as pltpu
from jax.sharding import PartitionSpec as P

TSTEPS = 1000
GROUPS = 6
TILE = 256
F32 = jnp.float32
BF16 = jnp.bfloat16


def plan_table(count):
    beta = 0.0001 + (0.02 - 0.0001) * np.arange(count, dtype=np.float64) / (count - 1)
    abar = np.cumprod(1.0 - beta)
    table = np.stack([beta / np.sqrt(1.0 - abar), 1.0 / np.sqrt(1.0 - beta), np.sqrt(beta)])
    return jnp.asarray(table.astype(np.float32))


def split3(x):
    high = x.astype(BF16).astype(F32)
    rest = x - high
    mid = rest.astype(BF16).astype(F32)
    return high, mid, rest - mid


def radices(count):
    found = []
    while count > 1:
        if count % 4 == 0 and (count.bit_length() - 1) % 2 == 0:
            radix = 4
        elif count % 2 == 0:
            radix = 2
        else:
            radix = count
        found.append(radix)
        count //= radix
    return found


def prep(start, slot, w_in, w_gate, w_value, w_down, w_out_t):
    lat, channels = w_in.shape
    prompts = start.shape[0]
    hidden = w_gate.shape[1]
    rows = lat + prompts
    half = channels // 2

    def body(start_ref, slot_ref, in_ref, gate_ref, value_ref, down_ref, out_ref, pack_ref, table_ref):
        lane = lax.broadcasted_iota(jnp.int32, (prompts, channels), 1)
        item = lax.broadcasted_iota(jnp.int32, (prompts, channels), 0)
        first_half = lane < half
        k = jnp.where(first_half, lane, lane - half).astype(F32)
        freq = jnp.exp(k * (-math.log(10000.0)) / half)
        times = jnp.zeros((prompts, channels), F32)
        for p in range(prompts):
            times = jnp.where(item == p, (start_ref[p] - slot_ref[0]).astype(F32), times)
        angle = times * freq
        emb = jnp.where(first_half, jnp.cos(angle), jnp.sin(angle))
        raw = jnp.concatenate([in_ref[...], emb], axis=0)
        centred = raw - jnp.sum(raw, axis=1, keepdims=True) * (1.0 / channels)
        place = lax.broadcasted_iota(jnp.int32, (rows, 128), 1)
        row_id = lax.broadcasted_iota(jnp.int32, (rows, 1), 0)
        table = jnp.zeros((rows, 128), F32)
        scale = channels ** -0.5
        rest = centred
        for s in range(lat):
            pivot = rest[s:s + 1]
            square = jnp.sum(pivot * pivot, axis=1, keepdims=True)
            pivot = pivot * jnp.where(square > 0, lax.rsqrt(square), 0.0)
            along = jnp.sum(rest * pivot, axis=1, keepdims=True)
            along = jnp.where(row_id >= s, along, 0.0)
            table = jnp.where(place == s, along * scale, table)
            rest = rest - along * pivot
        left = jnp.sqrt(jnp.sum(rest * rest, axis=1, keepdims=True))
        table = jnp.where(place == lat, left * scale, table)
        out_t = out_ref[...]
        for l in range(lat):
            base = jnp.sum(raw * out_t[l:l + 1], axis=1, keepdims=True)
            table = jnp.where(place == lat + 1 + l, base, table)
        table_ref[...] = table
        parts = jnp.concatenate(split3(centred), axis=0).astype(BF16)
        for i, weight_ref in enumerate((gate_ref, value_ref)):
            got = jnp.dot(parts, weight_ref[...], preferred_element_type=F32)
            got = got[:rows] + got[rows:2 * rows] + got[2 * rows:]
            pack_ref[i * rows:(i + 1) * rows] = got * math.sqrt(0.5)
        zero = jnp.zeros((rows - lat, channels), F32)
        wide = [jnp.concatenate([part, zero], axis=0) for part in split3(out_t)]
        parts = jnp.concatenate(wide, axis=0).astype(BF16)
        got = lax.dot_general(parts, down_ref[...], (((1,), (1,)), ((), ())), preferred_element_type=F32)
        pack_ref[2 * rows:] = got[:rows] + got[rows:2 * rows] + got[2 * rows:]

    smem = pl.BlockSpec(memory_space=pltpu.SMEM)
    vmem = pl.BlockSpec(memory_space=pltpu.VMEM)
    return pl.pallas_call(
        body,
        out_shape=(jax.ShapeDtypeStruct((3 * rows, hidden), F32), jax.ShapeDtypeStruct((rows, 128), F32)),
        in_specs=[smem, smem] + [vmem] * 5,
        out_specs=(vmem, vmem),
        name="prep",
    )(start, slot, w_in, w_gate, w_value, w_down, w_out_t)


def denoise(place, table, coef, latents, noise, packs):
    prompts, _, lat, pos = latents.shape
    peers, _, hidden = packs.shape
    rows = lat + prompts
    share = pos // peers
    tile = min(TILE, share)

    def body(place_ref, table_ref, coef_ref, lat_ref, noise_ref, pack_ref, term_ref, eps_ref, gate_lhs, value_lhs, fold_lhs):
        p = pl.program_id(0)

        @pl.when(p == 0)
        def _():
            for s in range(peers):
                for i, dest in enumerate((gate_lhs, value_lhs)):
                    high, mid, low = split3(pack_ref[s, i * rows:(i + 1) * rows])
                    stacked = jnp.concatenate([high, high, mid, high, low, mid], axis=0)
                    dest[s] = jnp.transpose(stacked).astype(BF16)
                high, mid, low = split3(pack_ref[s, 2 * rows:])
                pair = high + jnp.concatenate([mid[rows - lat:], mid[:rows - lat]], axis=0)
                fold_lhs[s] = jnp.concatenate([pair, low], axis=0).astype(BF16)

        mine = [lat_ref[0, 0, c:c + 1, :] for c in range(lat)]
        var = jnp.zeros((1, share), F32)
        for s in range(lat + 1):
            line = jnp.zeros((1, share), F32) + table_ref[lat + p, s]
            for c in range(s, lat):
                line = line + table_ref[c, s] * mine[c]
            var = var + line * line
        rstd = lax.rsqrt(var + 1e-05)
        lines = lax.broadcasted_iota(jnp.int32, (rows, share), 0)
        scaled = jnp.where(lines == lat + p, 1.0, 0.0)
        for c in range(lat):
            scaled = jnp.where(lines == c, mine[c], scaled)
        high, mid, low = split3(scaled * rstd)
        rhs = jnp.concatenate([high, mid, high, low, high, mid], axis=0).astype(BF16)
        outs = []
        for n in range(share // tile):
            cut = rhs[:, n * tile:(n + 1) * tile]
            total = jnp.zeros((2 * rows, tile), F32)
            for s in range(peers):
                gate = jnp.dot(gate_lhs[s], cut, preferred_element_type=F32)
                value = jnp.dot(value_lhs[s], cut, preferred_element_type=F32)
                act = (gate * value * (1.0 + lax.erf(gate))).astype(BF16)
                total = total + jnp.dot(fold_lhs[s], act, preferred_element_type=F32)
            outs.append(total[:lat] + total[rows - lat:rows] + total[rows:rows + lat])
        branch = jnp.concatenate(outs, axis=1)
        for l in range(lat):
            base = jnp.zeros((1, share), F32) + table_ref[lat + p, lat + 1 + l]
            for c in range(lat):
                base = base + table_ref[c, lat + 1 + l] * mine[c]
            eps = branch[l:l + 1] + base
            eps_ref[0, 0, l:l + 1, :] = eps
            stepped = (mine[l] - coef_ref[p, 0] * eps) * coef_ref[p, 1] + coef_ref[p, 2] * noise_ref[0, 0, l:l + 1, :]
            head = jnp.where(place_ref[1] == 0, mine[l], 0.0)
            term_ref[0, l:l + 1, :] = stepped - mine[l] + head

    smem = pl.BlockSpec(memory_space=pltpu.SMEM)
    grid_spec = pltpu.PrefetchScalarGridSpec(
        num_scalar_prefetch=1,
        grid=(prompts,),
        in_specs=[
            smem,
            smem,
            pl.BlockSpec((1, 1, lat, share), lambda p, place: (p, 0, 0, place[0])),
            pl.BlockSpec((1, 1, lat, share), lambda p, place: (p, 0, 0, place[0])),
            pl.BlockSpec(packs.shape, lambda p, place: (0, 0, 0)),
        ],
        out_specs=[
            pl.BlockSpec((1, lat, share), lambda p, place: (p, 0, 0)),
            pl.BlockSpec((1, 1, lat, share), lambda p, place: (p, 0, 0, 0)),
        ],
        scratch_shapes=[
            pltpu.VMEM((peers, hidden, GROUPS * rows), BF16),
            pltpu.VMEM((peers, hidden, GROUPS * rows), BF16),
            pltpu.VMEM((peers, 2 * rows, hidden), BF16),
        ],
    )
    return pl.pallas_call(
        body,
        grid_spec=grid_spec,
        out_shape=[
            jax.ShapeDtypeStruct((prompts, lat, share), F32),
            jax.ShapeDtypeStruct((prompts, 1, lat, share), F32),
        ],
        name="denoise",
    )(place, table, coef, latents, noise, packs)


def slid_sums(term, slide, axis):
    count = lax.axis_size(axis)
    mine = lax.axis_index(axis)

    def wanted(target, source):
        reach = jnp.minimum(target + slide, count - 1)
        return (source < reach)[:, None, None]

    digits = radices(count)
    below = 1
    held = None
    for radix in digits:
        digit = mine // below % radix

        def peer(i, k):
            d = i // below % radix
            return i + ((d + k) % radix - d) * below

        above = count // (below * radix)
        last_place = mine % (below * radix)
        if held is None:
            raws, sources = [term], [mine]
            for k in range(1, radix):
                raws.append(lax.ppermute(term, axis, [(i, peer(i, k)) for i in range(count)]))
                sources.append(peer(mine, radix - k))

            def partial(target):
                parts = [jnp.where(wanted(target, s), r, 0.0) for r, s in zip(raws, sources)]
                return sum(parts[1:], parts[0])

            held = partial
        else:
            earlier = held
            place = mine % below

            def offer(k):
                d = (digit + k) % radix
                return jnp.stack([earlier(place + d * below + a * below * radix) for a in range(above)])

            got = offer(0)
            for k in range(1, radix):
                got = got + lax.ppermute(offer(k), axis, [(i, peer(i, k)) for i in range(count)])

            def chosen(target, got=got, span=below * radix):
                if got.shape[0] == 1:
                    return got[0]
                return lax.dynamic_index_in_dim(got, target // span, 0, keepdims=False)

            held = chosen
        below *= radix
    if held is None:
        return jnp.where(wanted(mine, mine), term, 0.0)
    return held(mine)


def shards(latents, noise, start_step, slide, w_in, w_gate, w_value, w_down, w_out):
    prompts, t_dev, lat, pos = latents.shape
    assert t_dev == 1
    slot = lax.axis_index("tm").astype(jnp.int32)
    member = lax.axis_index("mp").astype(jnp.int32)
    pack, table = prep(start_step, slot[None], w_in, w_gate, w_value, w_down, w_out.T)
    packs = lax.all_gather(pack, "mp")
    plan = plan_table(TSTEPS)
    grid = jnp.arange(TSTEPS, dtype=jnp.int32)
    hit = (start_step - slot)[:, None, None] == grid
    coef = jnp.sum(jnp.where(hit, plan[None], 0.0), axis=-1)
    term, eps = denoise(jnp.stack([member, slot]), table, coef, latents, noise, packs)
    share = slid_sums(term, slide, "tm")
    result = lax.all_gather(share, "mp", axis=2, tiled=True)
    return result[:, None], eps


def solution(mesh):
    in_specs = (
        P(None, "tm", None, None),
        P(None, "tm", None, None),
        P(),
        P(),
        P(),
        P(None, "mp"),
        P(None, "mp"),
        P("mp", None),
        P(),
    )
    out_specs = (P(None, "tm", None, None), P(None, "tm", None, "mp"))
    return jax.shard_map(shards, mesh=mesh, in_specs=in_specs, out_specs=out_specs, check_vma=False)
```

```python
import math

import jax
import jax.numpy as jnp
import numpy as np
from jax import lax
from jax.experimental import pallas as pl
from jax.experimental.pallas import tpu as pltpu
from jax.sharding import PartitionSpec as P

TSTEPS = 1000
GROUPS = 6
VMEM_BYTES = 24 * 2**20
F32 = jnp.float32
BF16 = jnp.bfloat16


def plan_table(count):
    beta = 0.0001 + (0.02 - 0.0001) * np.arange(count, dtype=np.float64) / (count - 1)
    abar = np.cumprod(1.0 - beta)
    table = np.stack([beta / np.sqrt(1.0 - abar), 1.0 / np.sqrt(1.0 - beta), np.sqrt(beta)])
    wide = -count % 128
    return jnp.asarray(np.pad(table, ((0, 5), (0, wide))).astype(np.float32))


def split3(x):
    high = x.astype(BF16).astype(F32)
    rest = x - high
    mid = rest.astype(BF16).astype(F32)
    return high, mid, rest - mid


def radices(count):
    found = []
    while count > 1:
        if count % 4 == 0 and (count.bit_length() - 1) % 2 == 0:
            radix = 4
        elif count % 2 == 0:
            radix = 2
        else:
            radix = count
        found.append(radix)
        count //= radix
    return found


def params():
    return pltpu.CompilerParams(vmem_limit_bytes=VMEM_BYTES)


def cost(units):
    return pl.CostEstimate(flops=300 * units, transcendentals=units, bytes_accessed=0)


def project(start, slot, member, w_in, w_out_t, w_gate, w_value, w_down, latents, noise, share):
    lat, channels = w_in.shape
    prompts = start.shape[0]
    hidden = w_gate.shape[1]
    rows = lat + prompts
    half = channels // 2

    def body(start_ref, slot_ref, member_ref, in_ref, out_ref, *refs):
        gate_hbm, value_hbm, down_hbm, lat_hbm, noise_hbm = refs[:5]
        pack_ref, raw_ref, lat_ref, noise_ref, gate_ref, value_ref, down_ref, sems = refs[5:]
        cut = pl.ds(member_ref[0] * share, share)
        moves = [
            (gate_hbm, gate_ref),
            (value_hbm, value_ref),
            (down_hbm, down_ref),
            (lat_hbm.at[:, 0, :, cut], lat_ref),
            (noise_hbm.at[:, 0, :, cut], noise_ref),
        ]
        copies = [pltpu.make_async_copy(src, dst, sems.at[i]) for i, (src, dst) in enumerate(moves)]
        for copy in copies:
            copy.start()
        lane = lax.broadcasted_iota(jnp.int32, (prompts, channels), 1)
        item = lax.broadcasted_iota(jnp.int32, (prompts, channels), 0)
        first_half = lane < half
        k = jnp.where(first_half, lane, lane - half).astype(F32)
        freq = jnp.exp(k * (-math.log(10000.0)) / half)
        times = jnp.zeros((prompts, channels), F32)
        for p in range(prompts):
            times = jnp.where(item == p, (start_ref[p] - slot_ref[0]).astype(F32), times)
        angle = times * freq
        emb = jnp.where(first_half, jnp.cos(angle), jnp.sin(angle))
        raw = jnp.concatenate([in_ref[...], emb], axis=0)
        raw_ref[...] = raw
        centred = raw - jnp.sum(raw, axis=1, keepdims=True) * (1.0 / channels)
        parts = jnp.concatenate(split3(centred), axis=0).astype(BF16)
        for i, weight_ref in enumerate((gate_ref, value_ref)):
            copies[i].wait()
            got = jnp.dot(parts, weight_ref[...], preferred_element_type=F32)
            got = got[:rows] + got[rows:2 * rows] + got[2 * rows:]
            pack_ref[i * rows:(i + 1) * rows] = got * math.sqrt(0.5)
        zero = jnp.zeros((rows - lat, channels), F32)
        wide = [jnp.concatenate([part, zero], axis=0) for part in split3(out_ref[...])]
        parts = jnp.concatenate(wide, axis=0).astype(BF16)
        copies[2].wait()
        got = lax.dot_general(parts, down_ref[...], (((1,), (1,)), ((), ())), preferred_element_type=F32)
        pack_ref[2 * rows:] = got[:rows] + got[rows:2 * rows] + got[2 * rows:]
        for copy in copies[3:]:
            copy.wait()

    smem = pl.BlockSpec(memory_space=pltpu.SMEM)
    vmem = pl.BlockSpec(memory_space=pltpu.VMEM)
    hbm = pl.BlockSpec(memory_space=pltpu.HBM)
    return pl.pallas_call(
        body,
        out_shape=(
            jax.ShapeDtypeStruct((3 * rows, hidden), F32),
            jax.ShapeDtypeStruct((rows, channels), F32),
            jax.ShapeDtypeStruct((prompts, lat, share), F32),
            jax.ShapeDtypeStruct((prompts, lat, share), F32),
        ),
        in_specs=[smem] * 3 + [vmem] * 2 + [hbm] * 5,
        out_specs=(vmem,) * 4,
        scratch_shapes=[
            pltpu.VMEM(w_gate.shape, BF16),
            pltpu.VMEM(w_value.shape, BF16),
            pltpu.VMEM(w_down.shape, BF16),
            pltpu.SemaphoreType.DMA((5,)),
        ],
        compiler_params=params(),
        name="project",
    )(start, slot, member, w_in, w_out_t, *[pltpu.with_memory_space_constraint(x, pltpu.HBM) for x in (w_gate, w_value, w_down, latents, noise)])


def load_lhs(pack_ref, s, gate_lhs, value_lhs, fold_lhs, lat):
    rows = pack_ref.shape[1] // 3
    for i, dest in enumerate((gate_lhs, value_lhs)):
        high, mid, low = split3(pack_ref[s, i * rows:(i + 1) * rows])
        stacked = jnp.concatenate([high, high, mid, high, low, mid], axis=0)
        dest[s] = jnp.transpose(stacked).astype(BF16)
    high, mid, low = split3(pack_ref[s, 2 * rows:])
    pair = high + jnp.concatenate([mid[rows - lat:], mid[:rows - lat]], axis=0)
    fold_lhs[s] = jnp.concatenate([pair, low], axis=0).astype(BF16)


def hidden_sum(rhs, peers, gate_lhs, value_lhs, fold_lhs, lat):
    total = None
    for s in range(peers):
        gate = jnp.dot(gate_lhs[s], rhs, preferred_element_type=F32)
        value = jnp.dot(value_lhs[s], rhs, preferred_element_type=F32)
        act = (gate * value * (1.0 + lax.erf(gate))).astype(BF16)
        got = jnp.dot(fold_lhs[s], act, preferred_element_type=F32)
        total = got if total is None else total + got
    rows = total.shape[0] // 2
    return total[:lat] + total[rows - lat:rows] + total[rows:rows + lat]


def lhs_scratch(peers, rows, hidden):
    return [
        pltpu.VMEM((peers, hidden, GROUPS * rows), BF16),
        pltpu.VMEM((peers, hidden, GROUPS * rows), BF16),
        pltpu.VMEM((peers, 2 * rows, hidden), BF16),
    ]


def begin(start, slot, raw, w_out_t, plan, latents, packs):
    prompts, lat, share = latents.shape
    rows, channels = raw.shape
    peers, _, hidden = packs.shape

    def body(start_ref, slot_ref, raw_ref, out_ref, plan_ref, lat_ref, pack_ref, rhs_ref, eps_ref, coef_ref, gate_lhs, value_lhs, fold_lhs):
        for s in range(peers):
            load_lhs(pack_ref, s, gate_lhs, value_lhs, fold_lhs, lat)
        raw_rows = raw_ref[...]
        scale = channels ** -0.5
        rest = raw_rows - jnp.sum(raw_rows, axis=1, keepdims=True) * (1.0 / channels)
        row_id = lax.broadcasted_iota(jnp.int32, (rows, 1), 0)
        upper = []
        for s in range(lat):
            pivot = rest[s:s + 1]
            along = jnp.sum(rest * pivot, axis=1, keepdims=True)
            square = along[s:s + 1]
            inverse = jnp.where(square > 0, lax.rsqrt(square), 0.0)
            along = jnp.where(row_id >= s, along * inverse, 0.0)
            upper.append(along * scale)
            rest = rest - along * (pivot * inverse)
        left = jnp.sqrt(jnp.sum(rest * rest, axis=1, keepdims=True)) * scale
        out_t = out_ref[...]
        base = [jnp.sum(out_t * raw_rows[r:r + 1], axis=1, keepdims=True) for r in range(rows)]
        place = lax.broadcasted_iota(jnp.int32, plan_ref.shape, 1)
        lines = lax.broadcasted_iota(jnp.int32, (rows, share), 0)
        for p in range(prompts):
            hit = place == start_ref[p] - slot_ref[0]
            found = jnp.sum(jnp.where(hit, plan_ref[...], 0.0), axis=1, keepdims=True)
            coef_ref[p] = jnp.broadcast_to(found, coef_ref.shape[1:])
            mine = [lat_ref[p, c:c + 1, :] for c in range(lat)]
            var = left[lat + p:lat + p + 1] * left[lat + p:lat + p + 1]
            for s in range(lat):
                line = upper[s][lat + p:lat + p + 1]
                for c in range(s, lat):
                    line = line + upper[s][c:c + 1] * mine[c]
                var = var + line * line
            rstd = lax.rsqrt(var + 1e-05)
            scaled = jnp.where(lines == lat + p, 1.0, 0.0)
            for c in range(lat):
                scaled = jnp.where(lines == c, mine[c], scaled)
            high, mid, low = split3(scaled * rstd)
            rhs = jnp.concatenate([high, mid, high, low, high, mid], axis=0).astype(BF16)
            rhs_ref[p] = rhs
            eps = base[lat + p] + hidden_sum(rhs, peers, gate_lhs, value_lhs, fold_lhs, lat)
            for c in range(lat):
                eps = eps + base[c] * mine[c]
            eps_ref[p] = eps

    smem = pl.BlockSpec(memory_space=pltpu.SMEM)
    vmem = pl.BlockSpec(memory_space=pltpu.VMEM)
    return pl.pallas_call(
        body,
        out_shape=(
            jax.ShapeDtypeStruct((prompts, GROUPS * rows, share), BF16),
            jax.ShapeDtypeStruct((prompts, lat, share), F32),
            jax.ShapeDtypeStruct((prompts, plan.shape[0], 128), F32),
        ),
        in_specs=[smem] * 2 + [vmem] * 5,
        out_specs=(vmem,) * 3,
        scratch_shapes=lhs_scratch(peers, rows, hidden),
        compiler_params=params(),
        cost_estimate=cost(prompts * share * peers * hidden),
        name="begin",
    )(start, slot, raw, w_out_t, plan, latents, packs)


def extend(rhs, eps, packs):
    prompts, lat, share = eps.shape
    peers, rows, hidden = packs.shape

    def body(rhs_ref, eps_ref, pack_ref, out_ref, gate_lhs, value_lhs, fold_lhs):
        for s in range(peers):
            load_lhs(pack_ref, s, gate_lhs, value_lhs, fold_lhs, lat)
        for p in range(prompts):
            out_ref[p] = eps_ref[p] + hidden_sum(rhs_ref[p], peers, gate_lhs, value_lhs, fold_lhs, lat)

    vmem = pl.BlockSpec(memory_space=pltpu.VMEM)
    return pl.pallas_call(
        body,
        out_shape=jax.ShapeDtypeStruct(eps.shape, F32),
        in_specs=[vmem] * 3,
        out_specs=vmem,
        scratch_shapes=lhs_scratch(peers, rows // 3, hidden),
        compiler_params=params(),
        cost_estimate=cost(prompts * share * peers * hidden),
        name="extend",
    )(rhs, eps, packs)


def finish(slot, coef, latents, noise, rhs, eps, packs):
    prompts, lat, share = eps.shape
    peers, rows, hidden = packs.shape

    def body(slot_ref, coef_ref, lat_ref, noise_ref, rhs_ref, eps_ref, pack_ref, term_ref, out_ref, gate_lhs, value_lhs, fold_lhs):
        for s in range(peers):
            load_lhs(pack_ref, s, gate_lhs, value_lhs, fold_lhs, lat)
        for p in range(prompts):
            eps = eps_ref[p]
            if peers:
                eps = eps + hidden_sum(rhs_ref[p], peers, gate_lhs, value_lhs, fold_lhs, lat)
            out_ref[p, 0] = eps
            mine = lat_ref[p]
            weights = [coef_ref[p, i:i + 1, 0:1] for i in range(3)]
            stepped = (mine - weights[0] * eps) * weights[1] + weights[2] * noise_ref[p]
            term_ref[p] = stepped - mine + jnp.where(slot_ref[0] == 0, mine, 0.0)

    smem = pl.BlockSpec(memory_space=pltpu.SMEM)
    vmem = pl.BlockSpec(memory_space=pltpu.VMEM)
    return pl.pallas_call(
        body,
        out_shape=(
            jax.ShapeDtypeStruct(eps.shape, F32),
            jax.ShapeDtypeStruct((prompts, 1, lat, share), F32),
        ),
        in_specs=[smem] + [vmem] * 6,
        out_specs=(vmem,) * 2,
        scratch_shapes=lhs_scratch(peers, rows // 3, hidden),
        compiler_params=params(),
        cost_estimate=cost(prompts * share * peers * hidden),
        name="finish",
    )(slot, coef, latents, noise, rhs, eps, packs)


def slid_sums(term, slide, axis):
    count = lax.axis_size(axis)
    mine = lax.axis_index(axis)

    def wanted(target, source):
        reach = jnp.minimum(target + slide, count - 1)
        return (source < reach)[:, None, None]

    digits = radices(count)
    below = 1
    held = None
    for radix in digits:
        digit = mine // below % radix

        def peer(i, k):
            d = i // below % radix
            return i + ((d + k) % radix - d) * below

        above = count // (below * radix)
        last_place = mine % (below * radix)
        if held is None:
            raws, sources = [term], [mine]
            for k in range(1, radix):
                raws.append(lax.ppermute(term, axis, [(i, peer(i, k)) for i in range(count)]))
                sources.append(peer(mine, radix - k))

            def partial(target):
                parts = [jnp.where(wanted(target, s), r, 0.0) for r, s in zip(raws, sources)]
                return sum(parts[1:], parts[0])

            held = partial
        else:
            earlier = held
            place = mine % below

            def offer(k):
                d = (digit + k) % radix
                return jnp.stack([earlier(place + d * below + a * below * radix) for a in range(above)])

            got = offer(0)
            for k in range(1, radix):
                got = got + lax.ppermute(offer(k), axis, [(i, peer(i, k)) for i in range(count)])

            def chosen(target, got=got, span=below * radix):
                if got.shape[0] == 1:
                    return got[0]
                return lax.dynamic_index_in_dim(got, target // span, 0, keepdims=False)

            held = chosen
        below *= radix
    if held is None:
        return jnp.where(wanted(mine, mine), term, 0.0)
    return held(mine)


def swap(x, axis, step):
    count = lax.axis_size(axis)
    return lax.ppermute(x, axis, [(i, i ^ step) for i in range(count)])


def shards(latents, noise, start_step, slide, w_in, w_gate, w_value, w_down, w_out):
    prompts, t_dev, lat, pos = latents.shape
    assert t_dev == 1
    members = lax.axis_size("mp")
    share = pos // members
    slot = lax.axis_index("tm").astype(jnp.int32)[None]
    member = lax.axis_index("mp").astype(jnp.int32)[None]
    w_out_t = w_out.T
    plan = plan_table(TSTEPS)
    pack, raw, lat_share, noise_share = project(
        start_step, slot, member, w_in, w_out_t, w_gate, w_value, w_down, latents, noise, share
    )
    held = pack[None]
    step = members // 2
    arrived = swap(held, "mp", step) if step else None
    rhs, eps, coef = begin(start_step, slot, raw, w_out_t, plan, lat_share, held)
    while step > 1:
        arrived, rhs, eps = lax.optimization_barrier((arrived, rhs, eps))
        held = jnp.concatenate([held, arrived], axis=0)
        step //= 2
        following = swap(held, "mp", step)
        eps = extend(rhs, eps, arrived)
        arrived = following
    term, eps = finish(slot, coef, lat_share, noise_share, rhs, eps, arrived)
    result = slid_sums(term, slide, "tm")
    result = lax.all_gather(result, "mp", axis=2, tiled=True)
    return result[:, None], eps


def solution(mesh):
    in_specs = (
        P(None, "tm", None, None),
        P(None, "tm", None, None),
        P(),
        P(),
        P(),
        P(None, "mp"),
        P(None, "mp"),
        P("mp", None),
        P(),
    )
    out_specs = (P(None, "tm", None, None), P(None, "tm", None, "mp"))
    return jax.shard_map(shards, mesh=mesh, in_specs=in_specs, out_specs=out_specs, check_vma=False)
```
